32 devices in a mesh: grp: 2 (over x), wide: 16 (over z, y, core).
Axes of the slice: x: 2, y: 2, z: 4, core: 2. Of those that a mesh axis runs over, the one named last changes fastest.
Arguments:
- kv_prefill: bfloat16 [2, 16, 8, 8192, 128], P(None, 'grp', None, 'wide'), parts along dimension 1, may hold values from -4 to 4
- queries: bfloat16 [128, 1024], P(('grp', 'wide')), parts along dimension 0, may hold values from -512 to 512
- fresh_kv: bfloat16 [2, 128, 128], P(None, ('grp', 'wide')), parts along dimension 1, may hold values from -4 to 4
- lengths: int32 [16], P('grp'), parts along dimension 0, may hold values from 1 to 8191, as said below
- decode_slot_pair: int32 [128], P('grp'), parts along dimension 0, may hold values from 0 to 63, each once
Outputs:
- decode_cache: bfloat16 [2, 128, 8192, 128], P(None, ('grp', 'wide')), parts along dimension 1
- attention: bfloat16 [128, 1024], P(('grp', 'wide')), parts along dimension 0
The draws below stay inside these ranges and needn't reach their ends.
There are 2 independent parts, one for each index of `grp`. The reference program is written for one: setup_inputs(seed, part) draws one part's arguments, and reference() takes and returns one part's arrays. A program takes and returns all parts, laid end to end along the dimension named above; each array names one. Nothing has to cross between parts.
Inputs may be any that keep to these rules, and one draw needn't show every extreme that they name: `lengths`: every draw holds a sequence of length 8191 and one of length 1. `decode_slot_pair`: slot j lies on the device of wide with index j // (64 / 16).
All inputs are finite; a program needn't handle non-finite values.
Results may differ from the reference program's by a relative error of at most 0.001.
Values may be sent and summed in bfloat16 or wider, within the bound.
No kernel may reach another device: no remote copies, remote signals or barrier semaphores. Data moves between devices by JAX's collectives and lax.ppermute only.
A program may use at most 128 MiB of HBM per device.

```python
import math
import jax
import jax.numpy as jnp
from jax import lax

QUERY_HEADS = 64
KEY_VALUE_HEADS = 8
HEAD_SIZE = 128
GROUP_SEQUENCES = 8
CACHE_LENGTH = 8192
PAIR_COUNT = 64


def common_sample(key):
    every_key_row = jnp.clip(jax.random.normal(jax.random.fold_in(key, 11), (2, GROUP_SEQUENCES, KEY_VALUE_HEADS, CACHE_LENGTH, HEAD_SIZE), jnp.float32), -4.0, 4.0)
    every_query_row = jnp.clip(jax.random.normal(jax.random.fold_in(key, 12), (PAIR_COUNT, QUERY_HEADS // KEY_VALUE_HEADS, HEAD_SIZE), jnp.float32), -4.0, 4.0)
    fresh_all = jnp.clip(jax.random.normal(jax.random.fold_in(key, 13), (2, PAIR_COUNT, HEAD_SIZE), jnp.float32), -4.0, 4.0)
    return (every_key_row, every_query_row, fresh_all)


def draw_kv_prefill(key, part):
    return common_sample(key)[0].astype(jnp.bfloat16)


def draw_queries(key, part):
    return common_sample(key)[1].reshape(PAIR_COUNT, QUERY_HEADS // KEY_VALUE_HEADS * HEAD_SIZE).astype(jnp.bfloat16)


def draw_fresh_kv(key, part):
    return common_sample(key)[2].astype(jnp.bfloat16)


def draw_lengths(key, part):
    values = jax.random.randint(jax.random.fold_in(key, 21), (GROUP_SEQUENCES,), 1, CACHE_LENGTH, dtype=jnp.int32)
    order = jax.random.permutation(jax.random.fold_in(key, 22), GROUP_SEQUENCES)
    values = values.at[order[0]].set(CACHE_LENGTH - 1)
    values = values.at[order[1]].set(1)
    return values


def setup_inputs(seed: int = 0, part: int = 0) -> dict:
    splits = jax.random.split(jax.random.key(seed), 6)
    own_keys = jax.random.split(jax.random.fold_in(splits[5], part), 6)
    return {
        "kv_prefill": draw_kv_prefill(jax.random.fold_in(jax.random.fold_in(splits[5], part), 71), part),
        "queries": draw_queries(jax.random.fold_in(jax.random.fold_in(splits[5], part), 71), part),
        "fresh_kv": draw_fresh_kv(jax.random.fold_in(jax.random.fold_in(splits[5], part), 71), part),
        "lengths": draw_lengths(jax.random.fold_in(jax.random.fold_in(splits[5], part), 71), part),
        "decode_slot_pair": jax.random.permutation(own_keys[4], PAIR_COUNT).astype(jnp.int32),
    }


NEG_FILL = -1e+30

def reference(kv_prefill, queries, fresh_kv, lengths, decode_slot_pair):
    kv_items = kv_prefill.reshape(2, PAIR_COUNT, CACHE_LENGTH, HEAD_SIZE)
    positions = jnp.arange(CACHE_LENGTH, dtype=jnp.int32)
    pair_length = jnp.repeat(lengths, KEY_VALUE_HEADS)
    in_prompt = positions[None, :] < pair_length[:, None]
    cache_all = jnp.where(in_prompt[None, :, :, None], kv_items, jnp.zeros((), kv_items.dtype))
    at_new = positions[None, :] == pair_length[:, None]
    cache_all = jnp.where(at_new[None, :, :, None], fresh_kv[:, :, None, :], cache_all)
    decode_cache = jnp.take(cache_all, decode_slot_pair, axis=1)
    slot_len = jnp.take(pair_length, decode_slot_pair)
    decode_slot_query = jnp.take(queries, decode_slot_pair, axis=0).reshape(PAIR_COUNT, QUERY_HEADS // KEY_VALUE_HEADS, HEAD_SIZE)
    softmax_scale = 1.0 / math.sqrt(HEAD_SIZE)

    def attend_one(packed):
        query_rows, item_cache, limit = packed
        scores = jnp.dot(query_rows, item_cache[0].T, preferred_element_type=jnp.float32) * softmax_scale
        visible = positions <= limit
        scores = jnp.where(visible[None, :], scores, NEG_FILL)
        top_score = lax.optimization_barrier(jnp.max(scores, axis=1, keepdims=True))
        weights = jnp.where(visible[None, :], jnp.exp(scores - top_score), 0.0)
        total = lax.optimization_barrier(jnp.sum(weights, axis=1, keepdims=True))
        summed = jnp.dot(weights, item_cache[1].astype(jnp.float32), precision=lax.Precision.HIGHEST)
        return (summed / total).reshape(-1).astype(jnp.bfloat16)
    attention = lax.map(attend_one, (decode_slot_query, jnp.moveaxis(decode_cache, 1, 0), slot_len))
    return (decode_cache, attention)
```

```python
import functools
import math

import jax
import jax.numpy as jnp
from jax import lax
from jax.experimental import pallas as pl
from jax.experimental.pallas import tpu as pltpu
from jax.sharding import PartitionSpec as P

NEG_FILL = -1e30


def gather_body(me_ref, slots_ref, kv_ref, send_ref):
    send_ref[...] = kv_ref[...].reshape(send_ref.shape)


def gather_units(me, slots, kv, offset, per_device):
    _, _, rows, head_dim = kv.shape

    def pick(unit, me_ref, slots_ref):
        return (0, slots_ref[(me_ref[0] ^ offset) * per_device + unit], 0, 0)

    return pl.pallas_call(
        gather_body,
        out_shape=jax.ShapeDtypeStruct((per_device, 2, rows, head_dim), kv.dtype),
        grid_spec=pltpu.PrefetchScalarGridSpec(
            num_scalar_prefetch=2,
            grid=(per_device,),
            in_specs=[pl.BlockSpec((2, 1, rows, head_dim), pick)],
            out_specs=pl.BlockSpec((1, 2, rows, head_dim), lambda unit, *_: (unit, 0, 0, 0)),
        ),
        cost_estimate=pl.CostEstimate(
            flops=per_device * 2 * rows * head_dim * 16,
            bytes_accessed=4 * per_device * 2 * rows * head_dim,
            transcendentals=0,
        ),
        name="gather_units",
    )(me, slots, kv)


def absorb_body(
    offset, per_device, head_count, scale, first, me_ref, slots_ref, lengths_ref, recv_ref, token_ref, *refs
):
    if first:
        cache_ref, state_ref = refs
    else:
        _, old_ref, cache_ref, state_ref = refs
    slot = pl.program_id(0)
    me = me_ref[0]
    rows, head_dim = recv_ref.shape[-2:]
    group = state_ref.shape[2]
    item = slots_ref[me * per_device + slot]
    limit = lengths_ref[item // head_count] - (me ^ offset) * rows

    @pl.when(limit >= rows)
    def _():
        cache_ref[...] = recv_ref[...].reshape(cache_ref.shape)

    @pl.when(limit < 0)
    def _():
        cache_ref[...] = jnp.zeros_like(cache_ref)

    @pl.when((limit >= 0) & (limit < rows))
    def _():
        row = lax.broadcasted_iota(jnp.int32, (rows, head_dim), 0)
        for part in range(2):
            fresh = token_ref[0, group + part : group + part + 1, :].astype(jnp.float32)
            block = recv_ref[0, part].astype(jnp.float32)
            block = jnp.where(row < limit, block, jnp.where(row == limit, fresh, 0.0))
            cache_ref[part, 0] = block.astype(cache_ref.dtype)

    if first:
        old_max = jnp.full((group, head_dim), NEG_FILL, jnp.float32)
        old_sum = jnp.zeros((group, head_dim), jnp.float32)
        old_out = jnp.zeros((group, head_dim), jnp.float32)
    else:
        old_max, old_sum, old_out = old_ref[0, 0], old_ref[1, 0], old_ref[2, 0]

    @pl.when(limit < 0)
    def _():
        state_ref[0, 0] = old_max
        state_ref[1, 0] = old_sum
        state_ref[2, 0] = old_out

    @pl.when(limit >= 0)
    def _():
        query = token_ref[0, :group, :]
        scores = lax.dot_general(
            query, cache_ref[0, 0], (((1,), (1,)), ((), ())), preferred_element_type=jnp.float32
        )
        scores = scores * scale
        visible = lax.broadcasted_iota(jnp.int32, scores.shape, 1) <= limit
        scores = jnp.where(visible, scores, NEG_FILL)
        new_max = jnp.maximum(old_max, jnp.max(scores, axis=1, keepdims=True))
        weights = jnp.where(visible, jnp.exp(scores - new_max[:, :1]), 0.0)
        factor = jnp.exp(old_max - new_max)
        high = weights.astype(jnp.bfloat16)
        rest = weights - high.astype(jnp.float32)
        middle = rest.astype(jnp.bfloat16)
        low = (rest - middle.astype(jnp.float32)).astype(jnp.bfloat16)
        value = cache_ref[1, 0]
        summed = sum(
            jnp.dot(term, value, preferred_element_type=jnp.float32) for term in (low, middle, high)
        )
        state_ref[0, 0] = new_max
        state_ref[1, 0] = old_sum * factor + jnp.sum(weights, axis=1, keepdims=True)
        state_ref[2, 0] = old_out * factor + summed


def absorb(me, slots, lengths, recv, token_row, tokens, carry, offset, head_count, devices):
    per_device, _, rows, head_dim = recv.shape
    group = tokens.shape[1] - 2
    first = carry is None
    state_spec = pl.BlockSpec((3, 1, group, head_dim), lambda slot, *_: (0, slot, 0, 0))
    in_specs = [
        pl.BlockSpec((1, 2, rows, head_dim), lambda slot, *_: (slot, 0, 0, 0)),
        pl.BlockSpec(
            (1, group + 2, head_dim),
            lambda slot, me_ref, slots_ref, lengths_ref: (
                token_row(me_ref[0], slots_ref[me_ref[0] * per_device + slot]),
                0,
                0,
            ),
        ),
    ]
    if not first:
        in_specs += [pl.BlockSpec(memory_space=pl.ANY), state_spec]
    return pl.pallas_call(
        functools.partial(
            absorb_body, offset, per_device, head_count, 1.0 / math.sqrt(head_dim), first
        ),
        out_shape=[
            jax.ShapeDtypeStruct((2, per_device, rows * devices, head_dim), recv.dtype),
            jax.ShapeDtypeStruct((3, per_device, group, head_dim), jnp.float32),
        ],
        grid_spec=pltpu.PrefetchScalarGridSpec(
            num_scalar_prefetch=3,
            grid=(per_device,),
            in_specs=in_specs,
            out_specs=[
                pl.BlockSpec(
                    (2, 1, rows, head_dim), lambda slot, me_ref, *_: (0, slot, me_ref[0] ^ offset, 0)
                ),
                state_spec,
            ],
        ),
        input_output_aliases={} if first else {5: 0, 6: 1},
        cost_estimate=pl.CostEstimate(
            flops=per_device * 8 * group * rows * head_dim * 16,
            bytes_accessed=4 * per_device * 2 * rows * head_dim,
            transcendentals=per_device * group * rows,
        ),
        name="absorb",
    )(me, slots, lengths, recv, tokens, *(() if first else carry))


def local(kv_prefill, queries, fresh_kv, lengths, decode_slot_pair):
    devices = lax.axis_size("wide")
    seq_count, head_count, local_len, head_dim = kv_prefill.shape[1:]
    item_count = seq_count * head_count
    per_device = item_count // devices
    group_size = queries.shape[1] // head_dim
    me = lax.axis_index("wide").astype(jnp.int32).reshape(1)
    kv = kv_prefill.reshape(2, item_count, local_len, head_dim)
    tokens = jnp.concatenate(
        [queries.reshape(per_device, group_size, head_dim), jnp.swapaxes(fresh_kv, 0, 1)], axis=1
    )
    tokens = lax.all_gather(tokens, "wide", axis=0, tiled=True)

    def token_row(_, item):
        return item

    half = devices // 2
    order = [*range(half, devices), *range(half - 1, 0, -1)]
    arrived = {}
    for offset in order:
        sent = gather_units(me, decode_slot_pair, kv, offset, per_device)
        pairs = [(device, device ^ offset) for device in range(devices)]
        arrived[offset] = lax.ppermute(sent, "wide", pairs)
    arrived[0] = gather_units(me, decode_slot_pair, kv, 0, per_device)
    carry = None
    for offset in [0, *range(1, half), *range(half, devices)]:
        carry = absorb(
            me,
            decode_slot_pair,
            lengths,
            arrived[offset],
            token_row,
            tokens,
            carry,
            offset,
            head_count,
            devices,
        )
    decode_cache, state = carry
    attention = (state[2] / state[1]).reshape(per_device, group_size * head_dim)
    return (decode_cache, attention.astype(jnp.bfloat16))


def solution(mesh):
    in_specs = (
        P(None, "grp", None, "wide", None),
        P(("grp", "wide"), None),
        P(None, ("grp", "wide"), None),
        P("grp"),
        P("grp"),
    )
    out_specs = (P(None, ("grp", "wide"), None, None), P(("grp", "wide"), None))
    return jax.shard_map(local, mesh=mesh, in_specs=in_specs, out_specs=out_specs, check_vma=False)
```

```python
import functools
import math

import jax
import jax.numpy as jnp
from jax import lax
from jax.experimental import pallas as pl
from jax.experimental.pallas import tpu as pltpu
from jax.sharding import PartitionSpec as P

NEG_FILL = -1e30


def rank_of(limits, rows_start):
    held, ranks, count = [], [], 0
    for limit in limits:
        some = (limit > rows_start).astype(jnp.int32)
        held.append(some)
        ranks.append(count)
        count = count + some
    return held, ranks


def slot_lengths(slots_ref, lengths_ref, device, per_device, head_count):
    items = [slots_ref[device * per_device + slot] for slot in range(per_device)]
    return items, [lengths_ref[item // head_count] for item in items]


def gather_body(
    offset, per_device, head_count, dense, me_ref, slots_ref, lengths_ref, kv_ref, sent_ref, held_ref, in_sem, out_sem
):
    rows = kv_ref.shape[2]
    me = me_ref[0]
    items, limits = slot_lengths(slots_ref, lengths_ref, me ^ offset, per_device, head_count)
    held, ranks = rank_of(limits, me * rows)
    total = ranks[-1] + held[-1]
    for unit in range(per_device):
        if dense:
            item = items[unit]
        else:
            item = items[0]
            for slot in range(per_device):
                place = jnp.where(held[slot] == 1, ranks[slot], total + slot - ranks[slot])
                item = jnp.where(place == unit, items[slot], item)
        pltpu.make_async_copy(kv_ref.at[:, item], held_ref.at[unit], in_sem.at[unit]).start()
    for unit in range(per_device):
        pltpu.make_async_copy(kv_ref.at[:, 0], held_ref.at[unit], in_sem.at[unit]).wait()
        pltpu.make_async_copy(held_ref.at[unit], sent_ref.at[unit], out_sem.at[unit]).start()
    for unit in range(per_device):
        pltpu.make_async_copy(held_ref.at[unit], sent_ref.at[unit], out_sem.at[unit]).wait()


def gather_units(scalars, kv, offset, per_device, head_count, dense):
    _, _, rows, head_dim = kv.shape
    unit = (2, rows, head_dim)
    return pl.pallas_call(
        functools.partial(gather_body, offset, per_device, head_count, dense),
        out_shape=jax.ShapeDtypeStruct((per_device, *unit), kv.dtype),
        grid_spec=pltpu.PrefetchScalarGridSpec(
            num_scalar_prefetch=3,
            grid=(1,),
            in_specs=[pl.BlockSpec(memory_space=pl.ANY)],
            out_specs=pl.BlockSpec(memory_space=pl.ANY),
            scratch_shapes=[
                pltpu.VMEM((per_device, *unit), kv.dtype),
                pltpu.SemaphoreType.DMA((per_device,)),
                pltpu.SemaphoreType.DMA((per_device,)),
            ],
        ),
        cost_estimate=pl.CostEstimate(
            flops=per_device * 2 * rows * head_dim * 16,
            bytes_accessed=4 * per_device * 2 * rows * head_dim,
            transcendentals=0,
        ),
        name="gather_units",
    )(*scalars, kv)


def absorb_body(
    offset, per_device, head_count, scale, dense, first, me_ref, slots_ref, lengths_ref, recv_ref, *refs
):
    if first:
        token_ref, cache_ref, state_ref, held_ref, in_sem, out_sem = refs
    else:
        token_ref, _, old_ref, cache_ref, state_ref, held_ref, in_sem, out_sem = refs
    me = me_ref[0]
    rows, head_dim = held_ref.shape[-2:]
    group = state_ref.shape[2]
    start = (me ^ offset) * rows
    _, limits = slot_lengths(slots_ref, lengths_ref, me, per_device, head_count)
    held, ranks = rank_of(limits, start)
    for slot in range(per_device):
        unit = slot if dense else ranks[slot]

        @pl.when(held[slot] == 1)
        def _():
            pltpu.make_async_copy(recv_ref.at[unit], held_ref.at[slot], in_sem.at[slot]).start()

    for slot in range(per_device):
        limit = limits[slot] - start

        @pl.when(limit > 0)
        def _():
            pltpu.make_async_copy(recv_ref.at[0], held_ref.at[slot], in_sem.at[slot]).wait()

        @pl.when(limit <= 0)
        def _():
            held_ref[slot] = jnp.zeros_like(held_ref[slot])

        @pl.when((limit >= 0) & (limit < rows))
        def _():
            row = lax.broadcasted_iota(jnp.int32, (rows, head_dim), 0)
            for part in range(2):
                fresh = token_ref[slot, group + part : group + part + 1, :].astype(jnp.float32)
                block = held_ref[slot, part].astype(jnp.float32)
                block = jnp.where(row < limit, block, jnp.where(row == limit, fresh, 0.0))
                held_ref[slot, part] = block.astype(held_ref.dtype)

        for part in range(2):
            pltpu.make_async_copy(
                held_ref.at[slot, part],
                cache_ref.at[part, slot, pl.ds(pl.multiple_of(start, rows), rows)],
                out_sem.at[slot, part],
            ).start()

        if first:
            old_max = jnp.full((group, head_dim), NEG_FILL, jnp.float32)
            old_sum = jnp.zeros((group, head_dim), jnp.float32)
            old_out = jnp.zeros((group, head_dim), jnp.float32)
        else:
            old_max, old_sum, old_out = old_ref[0, slot], old_ref[1, slot], old_ref[2, slot]

        @pl.when(limit < 0)
        def _():
            state_ref[0, slot] = old_max
            state_ref[1, slot] = old_sum
            state_ref[2, slot] = old_out

        @pl.when(limit >= 0)
        def _():
            query = token_ref[slot, :group, :]
            scores = lax.dot_general(
                query, held_ref[slot, 0], (((1,), (1,)), ((), ())), preferred_element_type=jnp.float32
            )
            scores = scores * scale
            visible = lax.broadcasted_iota(jnp.int32, scores.shape, 1) <= limit
            scores = jnp.where(visible, scores, NEG_FILL)
            new_max = jnp.maximum(old_max, jnp.max(scores, axis=1, keepdims=True))
            weights = jnp.where(visible, jnp.exp(scores - new_max[:, :1]), 0.0)
            factor = jnp.exp(old_max - new_max)
            high = weights.astype(jnp.bfloat16)
            rest = weights - high.astype(jnp.float32)
            middle = rest.astype(jnp.bfloat16)
            low = (rest - middle.astype(jnp.float32)).astype(jnp.bfloat16)
            value = held_ref[slot, 1]
            summed = sum(
                jnp.dot(term, value, preferred_element_type=jnp.float32)
                for term in (low, middle, high)
            )
            state_ref[0, slot] = new_max
            state_ref[1, slot] = old_sum * factor + jnp.sum(weights, axis=1, keepdims=True)
            state_ref[2, slot] = old_out * factor + summed

    for slot in range(per_device):
        for part in range(2):
            pltpu.make_async_copy(
                held_ref.at[slot, part],
                cache_ref.at[part, slot, pl.ds(pl.multiple_of(start, rows), rows)],
                out_sem.at[slot, part],
            ).wait()


def absorb(scalars, recv, tokens, carry, offset, head_count, devices, dense):
    per_device, _, rows, head_dim = recv.shape
    group = tokens.shape[1] - 2
    first = carry is None
    anywhere, whole = pl.BlockSpec(memory_space=pl.ANY), pl.BlockSpec(memory_space=pltpu.VMEM)
    dtype = recv.dtype
    return pl.pallas_call(
        functools.partial(
            absorb_body, offset, per_device, head_count, 1.0 / math.sqrt(head_dim), dense, first
        ),
        out_shape=[
            jax.ShapeDtypeStruct((2, per_device, rows * devices, head_dim), dtype),
            jax.ShapeDtypeStruct((3, per_device, group, head_dim), jnp.float32),
        ],
        grid_spec=pltpu.PrefetchScalarGridSpec(
            num_scalar_prefetch=3,
            grid=(1,),
            in_specs=[anywhere, whole] + ([] if first else [anywhere, whole]),
            out_specs=[anywhere, whole],
            scratch_shapes=[
                pltpu.VMEM((per_device, 2, rows, head_dim), dtype),
                pltpu.SemaphoreType.DMA((per_device,)),
                pltpu.SemaphoreType.DMA((per_device, 2)),
            ],
        ),
        input_output_aliases={} if first else {5: 0, 6: 1},
        cost_estimate=pl.CostEstimate(
            flops=per_device * 8 * group * rows * head_dim * 16,
            bytes_accessed=4 * per_device * 2 * rows * head_dim,
            transcendentals=per_device * group * rows,
        ),
        name="absorb",
    )(*scalars, recv, tokens, *(() if first else carry))


def swap_units(units, pairs, count):
    def body(unit, held):
        sent = lax.dynamic_index_in_dim(held, unit, keepdims=False)
        return lax.dynamic_update_index_in_dim(held, lax.ppermute(sent, "wide", pairs), unit, 0)

    return lax.fori_loop(0, count, body, units)


def local(kv_prefill, queries, fresh_kv, lengths, decode_slot_pair):
    devices = lax.axis_size("wide")
    seq_count, head_count, local_len, head_dim = kv_prefill.shape[1:]
    item_count = seq_count * head_count
    per_device = item_count // devices
    group_size = queries.shape[1] // head_dim
    rank = lax.axis_index("wide").astype(jnp.int32)
    kv = kv_prefill.reshape(2, item_count, local_len, head_dim)
    tokens = jnp.concatenate(
        [queries.reshape(per_device, group_size, head_dim), jnp.swapaxes(fresh_kv, 0, 1)], axis=1
    )
    scalars = (rank.reshape(1), decode_slot_pair, lengths)

    def pairs_of(offset):
        return [(device, device ^ offset) for device in range(devices)]

    stride = 1
    while stride < devices:
        steps = min(4, devices // stride)
        blocks = [
            lax.ppermute(tokens, "wide", pairs_of(step * stride)) for step in range(1, steps)
        ]
        tokens = jnp.concatenate([tokens, *blocks], axis=0)
        stride *= steps
    half = devices // 2
    quarter = max(half // 2, 1)
    near = [*range(quarter, half), *range(1, quarter)]
    far = [*range(half, devices)]
    arrived = {}
    dense = {offset: True for offset in range(devices)}
    order = [
        *(offset for both in zip(far[:quarter], near[:quarter]) for offset in both),
        *near[quarter:],
        *far[quarter:],
    ]
    ready = {
        offset: gather_units(scalars, kv, offset, per_device, head_count, True) for offset in order[:2]
    }
    tokens, rank_after, ready = lax.optimization_barrier((tokens, rank, ready))
    scalars = (rank_after.reshape(1), decode_slot_pair, lengths)
    for offset in order:
        if offset not in ready:
            ready[offset] = gather_units(scalars, kv, offset, per_device, head_count, True)
        arrived[offset] = lax.ppermute(ready[offset], "wide", pairs_of(offset))
    arrived[0] = gather_units(scalars, kv, 0, per_device, head_count, True)
    own_slots = lax.dynamic_slice_in_dim(decode_slot_pair, rank * per_device, per_device)
    rows = ((own_slots // per_device) ^ rank) * per_device + own_slots % per_device
    own_tokens = jnp.take(tokens, rows, axis=0)

    carry = None
    for offset in [0, *order]:
        carry = absorb(
            scalars, arrived[offset], own_tokens, carry, offset, head_count, devices, dense[offset]
        )
    decode_cache, state = carry
    attention = (state[2] / state[1]).reshape(per_device, group_size * head_dim)
    return (decode_cache, attention.astype(jnp.bfloat16))


def solution(mesh):
    in_specs = (
        P(None, "grp", None, "wide", None),
        P(("grp", "wide"), None),
        P(None, ("grp", "wide"), None),
        P("grp"),
        P("grp"),
    )
    out_specs = (P(None, ("grp", "wide"), None, None), P(("grp", "wide"), None))
    return jax.shard_map(local, mesh=mesh, in_specs=in_specs, out_specs=out_specs, check_vma=False)
```

```python
import functools
import math

import jax
import jax.numpy as jnp
from jax import lax
from jax.experimental import pallas as pl
from jax.experimental.pallas import tpu as pltpu
from jax.sharding import PartitionSpec as P

NEG_FILL = -1e30


def rank_of(limits, rows_start):
    held, ranks, count = [], [], 0
    for limit in limits:
        some = (limit > rows_start).astype(jnp.int32)
        held.append(some)
        ranks.append(count)
        count = count + some
    return held, ranks


def slot_lengths(slots_ref, lengths_ref, device, per_device, head_count):
    items = [slots_ref[device * per_device + slot] for slot in range(per_device)]
    return items, [lengths_ref[item // head_count] for item in items]


def gather_body(
    offset, per_device, head_count, dense, me_ref, slots_ref, lengths_ref, kv_ref, sent_ref, held_ref, in_sem, out_sem
):
    rows = kv_ref.shape[2]
    me = me_ref[0]
    items, limits = slot_lengths(slots_ref, lengths_ref, me ^ offset, per_device, head_count)
    held, ranks = rank_of(limits, me * rows)
    total = ranks[-1] + held[-1]
    for unit in range(per_device):
        if dense:
            item = items[unit]
        else:
            item = items[0]
            for slot in range(per_device):
                place = jnp.where(held[slot] == 1, ranks[slot], total + slot - ranks[slot])
                item = jnp.where(place == unit, items[slot], item)
        pltpu.make_async_copy(kv_ref.at[:, item], held_ref.at[unit], in_sem.at[unit]).start()
    for unit in range(per_device):
        pltpu.make_async_copy(kv_ref.at[:, 0], held_ref.at[unit], in_sem.at[unit]).wait()
        pltpu.make_async_copy(held_ref.at[unit], sent_ref.at[unit], out_sem.at[unit]).start()
    for unit in range(per_device):
        pltpu.make_async_copy(held_ref.at[unit], sent_ref.at[unit], out_sem.at[unit]).wait()


def gather_units(scalars, kv, offset, per_device, head_count, dense):
    _, _, rows, head_dim = kv.shape
    unit = (2, rows, head_dim)
    return pl.pallas_call(
        functools.partial(gather_body, offset, per_device, head_count, dense),
        out_shape=jax.ShapeDtypeStruct((per_device, *unit), kv.dtype),
        grid_spec=pltpu.PrefetchScalarGridSpec(
            num_scalar_prefetch=3,
            grid=(1,),
            in_specs=[pl.BlockSpec(memory_space=pl.ANY)],
            out_specs=pl.BlockSpec(memory_space=pl.ANY),
            scratch_shapes=[
                pltpu.VMEM((per_device, *unit), kv.dtype),
                pltpu.SemaphoreType.DMA((per_device,)),
                pltpu.SemaphoreType.DMA((per_device,)),
            ],
        ),
        cost_estimate=pl.CostEstimate(
            flops=per_device * 2 * rows * head_dim * 16,
            bytes_accessed=4 * per_device * 2 * rows * head_dim,
            transcendentals=0,
        ),
        name="gather_units",
    )(*scalars, kv)


def absorb_body(
    offset, per_device, head_count, scale, dense, first, last, me_ref, slots_ref, lengths_ref, recv_ref, *refs
):
    if first:
        token_ref, cache_ref, state_ref, held_ref, in_sem, out_sem = refs
    else:
        token_ref, _, old_ref, cache_ref, state_ref, held_ref, in_sem, out_sem = refs
    me = me_ref[0]
    rows, head_dim = held_ref.shape[-2:]
    group = token_ref.shape[1] - 2
    start = (me ^ offset) * rows
    _, limits = slot_lengths(slots_ref, lengths_ref, me, per_device, head_count)
    held, ranks = rank_of(limits, start)
    for slot in range(per_device):
        unit = slot if dense else ranks[slot]

        @pl.when(held[slot] == 1)
        def _():
            pltpu.make_async_copy(recv_ref.at[unit], held_ref.at[slot], in_sem.at[slot]).start()

    for slot in range(per_device):
        limit = limits[slot] - start

        @pl.when(limit > 0)
        def _():
            pltpu.make_async_copy(recv_ref.at[0], held_ref.at[slot], in_sem.at[slot]).wait()

        @pl.when(limit <= 0)
        def _():
            held_ref[slot] = jnp.zeros_like(held_ref[slot])

        @pl.when((limit >= 0) & (limit < rows))
        def _():
            row = lax.broadcasted_iota(jnp.int32, (rows, head_dim), 0)
            for part in range(2):
                fresh = token_ref[slot, group + part : group + part + 1, :].astype(jnp.float32)
                block = held_ref[slot, part].astype(jnp.float32)
                block = jnp.where(row < limit, block, jnp.where(row == limit, fresh, 0.0))
                held_ref[slot, part] = block.astype(held_ref.dtype)

        for part in range(2):
            pltpu.make_async_copy(
                held_ref.at[slot, part],
                cache_ref.at[part, slot, pl.ds(pl.multiple_of(start, rows), rows)],
                out_sem.at[slot, part],
            ).start()

    outputs = []
    for slot in range(per_device):
        limit = limits[slot] - start
        if first:
            old_max = jnp.full((group, head_dim), NEG_FILL, jnp.float32)
            old_sum = jnp.zeros((group, head_dim), jnp.float32)
            old_out = jnp.zeros((group, head_dim), jnp.float32)
        else:
            old_max, old_sum, old_out = old_ref[0, slot], old_ref[1, slot], old_ref[2, slot]
        query = token_ref[slot, :group, :]
        scores = lax.dot_general(
            query, held_ref[slot, 0], (((1,), (1,)), ((), ())), preferred_element_type=jnp.float32
        )
        scores = scores * scale
        visible = lax.broadcasted_iota(jnp.int32, scores.shape, 1) <= limit
        scores = jnp.where(visible, scores, NEG_FILL)
        new_max = jnp.maximum(old_max, jnp.max(scores, axis=1, keepdims=True))
        weights = jnp.where(visible, jnp.exp(scores - new_max[:, :1]), 0.0)
        factor = jnp.exp(old_max - new_max)
        high = weights.astype(jnp.bfloat16)
        rest = weights - high.astype(jnp.float32)
        middle = rest.astype(jnp.bfloat16)
        low = (rest - middle.astype(jnp.float32)).astype(jnp.bfloat16)
        value = held_ref[slot, 1]
        summed = sum(
            jnp.dot(term, value, preferred_element_type=jnp.float32) for term in (low, middle, high)
        )
        new_sum = old_sum * factor + jnp.sum(weights, axis=1, keepdims=True)
        new_out = old_out * factor + summed
        if last:
            mean = new_out / new_sum
            heads = [mean[head : head + 1] for head in range(group)]
            outputs.append(jnp.concatenate(heads, axis=1))
        else:
            state_ref[0, slot] = new_max
            state_ref[1, slot] = new_sum
            state_ref[2, slot] = new_out
    if last:
        state_ref[...] = jnp.concatenate(outputs, axis=0).astype(state_ref.dtype)

    for slot in range(per_device):
        for part in range(2):
            pltpu.make_async_copy(
                held_ref.at[slot, part],
                cache_ref.at[part, slot, pl.ds(pl.multiple_of(start, rows), rows)],
                out_sem.at[slot, part],
            ).wait()


def absorb(scalars, recv, tokens, carry, offset, head_count, devices, dense, last):
    per_device, _, rows, head_dim = recv.shape
    group = tokens.shape[1] - 2
    first = carry is None
    anywhere, whole = pl.BlockSpec(memory_space=pl.ANY), pl.BlockSpec(memory_space=pltpu.VMEM)
    dtype = recv.dtype
    return pl.pallas_call(
        functools.partial(
            absorb_body, offset, per_device, head_count, 1.0 / math.sqrt(head_dim), dense, first, last
        ),
        out_shape=[
            jax.ShapeDtypeStruct((2, per_device, rows * devices, head_dim), dtype),
            jax.ShapeDtypeStruct((per_device, group * head_dim), dtype)
            if last
            else jax.ShapeDtypeStruct((3, per_device, group, head_dim), jnp.float32),
        ],
        grid_spec=pltpu.PrefetchScalarGridSpec(
            num_scalar_prefetch=3,
            grid=(1,),
            in_specs=[anywhere, whole] + ([] if first else [anywhere, whole]),
            out_specs=[anywhere, whole],
            scratch_shapes=[
                pltpu.VMEM((per_device, 2, rows, head_dim), dtype),
                pltpu.SemaphoreType.DMA((per_device,)),
                pltpu.SemaphoreType.DMA((per_device, 2)),
            ],
        ),
        input_output_aliases={} if first else {5: 0} if last else {5: 0, 6: 1},
        cost_estimate=pl.CostEstimate(
            flops=per_device * 8 * group * rows * head_dim * 16,
            bytes_accessed=4 * per_device * 2 * rows * head_dim,
            transcendentals=per_device * group * rows,
        ),
        name="absorb",
    )(*scalars, recv, tokens, *(() if first else carry))


def local(kv_prefill, queries, fresh_kv, lengths, decode_slot_pair):
    devices = lax.axis_size("wide")
    seq_count, head_count, local_len, head_dim = kv_prefill.shape[1:]
    item_count = seq_count * head_count
    per_device = item_count // devices
    group_size = queries.shape[1] // head_dim
    rank = lax.axis_index("wide").astype(jnp.int32)
    kv = kv_prefill.reshape(2, item_count, local_len, head_dim)
    scalars = (rank.reshape(1), decode_slot_pair, lengths)

    def pairs_of(offset):
        return [(device, device ^ offset) for device in range(devices)]

    def go_round(tokens, stride, steps):
        blocks = [
            lax.ppermute(tokens, "wide", pairs_of(step * stride)) for step in range(1, steps)
        ]
        return jnp.concatenate([tokens, *blocks], axis=0)

    half = devices // 2
    quarter = max(half // 2, 1)
    near = [*range(quarter, half), *range(1, quarter)]
    far = [*range(half, devices)]
    arrived = {}
    dense = {offset: True for offset in range(devices)}
    order = [
        *(offset for both in zip(far[:quarter], near[:quarter]) for offset in both),
        *near[quarter:],
        *far[quarter:],
    ]
    early = 1
    for offset in order[:early]:
        units = gather_units(scalars, kv, offset, per_device, head_count, True)
        arrived[offset] = lax.ppermute(units, "wide", pairs_of(offset))
    units, queries, fresh_kv = lax.optimization_barrier((units, queries, fresh_kv))
    tokens = jnp.concatenate(
        [queries.reshape(per_device, group_size, head_dim), jnp.swapaxes(fresh_kv, 0, 1)], axis=1
    )
    stride = min(4, devices)
    tokens = go_round(tokens, 1, stride)
    while stride < devices:
        steps = min(4, devices // stride)
        tokens = go_round(tokens, stride, steps)
        stride *= steps
    for offset in order[early:]:
        units = gather_units(scalars, kv, offset, per_device, head_count, True)
        arrived[offset] = lax.ppermute(units, "wide", pairs_of(offset))
    arrived[0] = gather_units(scalars, kv, 0, per_device, head_count, True)
    own_slots = lax.dynamic_slice_in_dim(decode_slot_pair, rank * per_device, per_device)
    rows = ((own_slots // per_device) ^ rank) * per_device + own_slots % per_device
    own_tokens = jnp.take(tokens, rows, axis=0)

    carry = None
    for offset in [0, *order]:
        carry = absorb(
            scalars,
            arrived[offset],
            own_tokens,
            carry,
            offset,
            head_count,
            devices,
            dense[offset],
            offset == order[-1],
        )
    return tuple(carry)


def solution(mesh):
    in_specs = (
        P(None, "grp", None, "wide", None),
        P(("grp", "wide"), None),
        P(None, ("grp", "wide"), None),
        P("grp"),
        P("grp"),
    )
    out_specs = (P(None, ("grp", "wide"), None, None), P(("grp", "wide"), None))

    return jax.shard_map(local, mesh=mesh, in_specs=in_specs, out_specs=out_specs, check_vma=False)
```

```python
import functools
import math

import jax
import jax.numpy as jnp
from jax import lax
from jax.experimental import pallas as pl
from jax.experimental.pallas import tpu as pltpu
from jax.sharding import PartitionSpec as P

NEG_FILL = -1e30


def rank_of(limits, rows_start):
    held, ranks, count = [], [], 0
    for limit in limits:
        some = (limit > rows_start).astype(jnp.int32)
        held.append(some)
        ranks.append(count)
        count = count + some
    return held, ranks


def slot_lengths(slots_ref, lengths_ref, device, per_device, head_count):
    items = [slots_ref[device * per_device + slot] for slot in range(per_device)]
    return items, [lengths_ref[item // head_count] for item in items]


def gather_body(
    offset, per_device, head_count, dense, me_ref, slots_ref, lengths_ref, kv_ref, *refs
):
    *outs, held_ref, in_sem, out_sem = refs
    places = [ref.at[unit] for ref in outs for unit in range(ref.shape[0])]
    rows = kv_ref.shape[2]
    me = me_ref[0]
    items, limits = slot_lengths(slots_ref, lengths_ref, me ^ offset, per_device, head_count)
    held, ranks = rank_of(limits, me * rows)
    total = ranks[-1] + held[-1]
    for unit in range(per_device):
        if dense:
            item = items[unit]
        else:
            item = items[0]
            for slot in range(per_device):
                place = jnp.where(held[slot] == 1, ranks[slot], total + slot - ranks[slot])
                item = jnp.where(place == unit, items[slot], item)
        pltpu.make_async_copy(kv_ref.at[:, item], held_ref.at[unit], in_sem.at[unit]).start()
    for unit in range(per_device):
        pltpu.make_async_copy(kv_ref.at[:, 0], held_ref.at[unit], in_sem.at[unit]).wait()
        pltpu.make_async_copy(held_ref.at[unit], places[unit], out_sem.at[unit]).start()
    for unit in range(per_device):
        pltpu.make_async_copy(held_ref.at[unit], places[unit], out_sem.at[unit]).wait()


def gather_units(scalars, kv, offset, parts, head_count, dense):
    _, _, rows, head_dim = kv.shape
    unit, per_device = (2, rows, head_dim), sum(parts)
    return pl.pallas_call(
        functools.partial(gather_body, offset, per_device, head_count, dense),
        out_shape=[jax.ShapeDtypeStruct((part, *unit), kv.dtype) for part in parts],
        grid_spec=pltpu.PrefetchScalarGridSpec(
            num_scalar_prefetch=3,
            grid=(1,),
            in_specs=[pl.BlockSpec(memory_space=pl.ANY)],
            out_specs=[pl.BlockSpec(memory_space=pl.ANY)] * len(parts),
            scratch_shapes=[
                pltpu.VMEM((per_device, *unit), kv.dtype),
                pltpu.SemaphoreType.DMA((per_device,)),
                pltpu.SemaphoreType.DMA((per_device,)),
            ],
        ),
        cost_estimate=pl.CostEstimate(
            flops=per_device * 2 * rows * head_dim * 16,
            bytes_accessed=4 * per_device * 2 * rows * head_dim,
            transcendentals=0,
        ),
        name="gather_units",
    )(*scalars, kv)


def heads_side_by_side(mean):
    return jnp.concatenate([mean[head : head + 1] for head in range(mean.shape[0])], axis=1)


def absorb_body(
    offset, per_device, head_count, scale, dense, first, last, active, me_ref, slots_ref, lengths_ref, recv_ref, *refs
):
    if first:
        token_ref, cache_ref, state_ref, held_ref, in_sem, out_sem = refs
    else:
        token_ref, _, old_ref, cache_ref, state_ref, held_ref, in_sem, out_sem = refs
    me = me_ref[0]
    rows, head_dim = held_ref.shape[-2:]
    group = token_ref.shape[1] - 2
    start = (me ^ offset) * rows
    _, limits = slot_lengths(slots_ref, lengths_ref, me, per_device, head_count)
    held, ranks = rank_of(limits, start)
    for slot in active:
        unit = slot - active[0] if dense else ranks[slot]

        @pl.when(held[slot] == 1)
        def _():
            pltpu.make_async_copy(recv_ref.at[unit], held_ref.at[slot - active[0]], in_sem.at[slot]).start()

    for slot in active:
        limit = limits[slot] - start

        @pl.when(limit > 0)
        def _():
            pltpu.make_async_copy(recv_ref.at[0], held_ref.at[slot - active[0]], in_sem.at[slot]).wait()

        @pl.when(limit <= 0)
        def _():
            held_ref[slot - active[0]] = jnp.zeros_like(held_ref[slot - active[0]])

        @pl.when((limit >= 0) & (limit < rows))
        def _():
            row = lax.broadcasted_iota(jnp.int32, (rows, head_dim), 0)
            for part in range(2):
                fresh = token_ref[slot, group + part : group + part + 1, :].astype(jnp.float32)
                block = held_ref[slot - active[0], part].astype(jnp.float32)
                block = jnp.where(row < limit, block, jnp.where(row == limit, fresh, 0.0))
                held_ref[slot - active[0], part] = block.astype(held_ref.dtype)

        for part in range(2):
            pltpu.make_async_copy(
                held_ref.at[slot - active[0], part],
                cache_ref.at[part, slot, pl.ds(pl.multiple_of(start, rows), rows)],
                out_sem.at[slot, part],
            ).start()

    outputs = []
    for slot in range(per_device):
        limit = limits[slot] - start
        if first:
            old_max = jnp.full((group, head_dim), NEG_FILL, jnp.float32)
            old_sum = jnp.zeros((group, head_dim), jnp.float32)
            old_out = jnp.zeros((group, head_dim), jnp.float32)
        else:
            old_max, old_sum, old_out = old_ref[0, slot], old_ref[1, slot], old_ref[2, slot]
        if slot not in active:
            if last:
                outputs.append(heads_side_by_side(old_out / old_sum))
            else:
                state_ref[0, slot] = old_max
                state_ref[1, slot] = old_sum
                state_ref[2, slot] = old_out
            continue
        query = token_ref[slot, :group, :]
        scores = lax.dot_general(
            query, held_ref[slot - active[0], 0], (((1,), (1,)), ((), ())), preferred_element_type=jnp.float32
        )
        scores = scores * scale
        visible = lax.broadcasted_iota(jnp.int32, scores.shape, 1) <= limit
        scores = jnp.where(visible, scores, NEG_FILL)
        new_max = jnp.maximum(old_max, jnp.max(scores, axis=1, keepdims=True))
        weights = jnp.where(visible, jnp.exp(scores - new_max[:, :1]), 0.0)
        factor = jnp.exp(old_max - new_max)
        high = weights.astype(jnp.bfloat16)
        rest = weights - high.astype(jnp.float32)
        middle = rest.astype(jnp.bfloat16)
        low = (rest - middle.astype(jnp.float32)).astype(jnp.bfloat16)
        value = held_ref[slot - active[0], 1]
        summed = sum(
            jnp.dot(term, value, preferred_element_type=jnp.float32) for term in (low, middle, high)
        )
        new_sum = old_sum * factor + jnp.sum(weights, axis=1, keepdims=True)
        new_out = old_out * factor + summed
        if last:
            outputs.append(heads_side_by_side(new_out / new_sum))
        else:
            state_ref[0, slot] = new_max
            state_ref[1, slot] = new_sum
            state_ref[2, slot] = new_out
    if last:
        state_ref[...] = jnp.concatenate(outputs, axis=0).astype(state_ref.dtype)

    for slot in active:
        for part in range(2):
            pltpu.make_async_copy(
                held_ref.at[slot - active[0], part],
                cache_ref.at[part, slot, pl.ds(pl.multiple_of(start, rows), rows)],
                out_sem.at[slot, part],
            ).wait()


def absorb(scalars, recv, tokens, carry, offset, head_count, devices, dense, last, active):
    _, _, rows, head_dim = recv.shape
    per_device = tokens.shape[0]
    group = tokens.shape[1] - 2
    first = carry is None
    anywhere, whole = pl.BlockSpec(memory_space=pl.ANY), pl.BlockSpec(memory_space=pltpu.VMEM)
    dtype = recv.dtype
    return pl.pallas_call(
        functools.partial(
            absorb_body, offset, per_device, head_count, 1.0 / math.sqrt(head_dim), dense, first, last, active
        ),
        out_shape=[
            jax.ShapeDtypeStruct((2, per_device, rows * devices, head_dim), dtype),
            jax.ShapeDtypeStruct((per_device, group * head_dim), dtype)
            if last
            else jax.ShapeDtypeStruct((3, per_device, group, head_dim), jnp.float32),
        ],
        grid_spec=pltpu.PrefetchScalarGridSpec(
            num_scalar_prefetch=3,
            grid=(1,),
            in_specs=[anywhere, whole] + ([] if first else [anywhere, whole]),
            out_specs=[anywhere, whole],
            scratch_shapes=[
                pltpu.VMEM((len(active), 2, rows, head_dim), dtype),
                pltpu.SemaphoreType.DMA((per_device,)),
                pltpu.SemaphoreType.DMA((per_device, 2)),
            ],
        ),
        input_output_aliases={} if first else {5: 0} if last else {5: 0, 6: 1},
        cost_estimate=pl.CostEstimate(
            flops=per_device * 8 * group * rows * head_dim * 16,
            bytes_accessed=4 * per_device * 2 * rows * head_dim,
            transcendentals=per_device * group * rows,
        ),
        name="absorb",
    )(*scalars, recv, tokens, *(() if first else carry))


def local(kv_prefill, queries, fresh_kv, lengths, decode_slot_pair):
    devices = lax.axis_size("wide")
    seq_count, head_count, local_len, head_dim = kv_prefill.shape[1:]
    item_count = seq_count * head_count
    per_device = item_count // devices
    group_size = queries.shape[1] // head_dim
    rank = lax.axis_index("wide").astype(jnp.int32)
    kv = kv_prefill.reshape(2, item_count, local_len, head_dim)
    scalars = (rank.reshape(1), decode_slot_pair, lengths)

    def pairs_of(offset):
        return [(device, device ^ offset) for device in range(devices)]

    def go_round(tokens, stride, steps):
        blocks = [
            lax.ppermute(tokens, "wide", pairs_of(step * stride)) for step in range(1, steps)
        ]
        return jnp.concatenate([tokens, *blocks], axis=0)

    half = devices // 2
    quarter = max(half // 2, 1)
    near = [*range(quarter, half), *range(1, quarter)]
    far = [*range(half, devices)]
    arrived = {}
    dense = {offset: True for offset in range(devices)}
    order = [
        *(offset for both in zip(far[:quarter], near[:quarter]) for offset in both),
        *near[quarter:],
        *far[quarter:],
    ]

    def parts_of(offset):
        first = (per_device + 1) // 2
        split = offset == order[-1] and per_device > 1
        return [first, per_device - first] if split else [per_device]

    early = 1
    for offset in order[:early]:
        units = gather_units(scalars, kv, offset, parts_of(offset), head_count, True)
        arrived[offset] = [lax.ppermute(part, "wide", pairs_of(offset)) for part in units]
    units, queries, fresh_kv = lax.optimization_barrier((units, queries, fresh_kv))
    tokens = jnp.concatenate(
        [queries.reshape(per_device, group_size, head_dim), jnp.swapaxes(fresh_kv, 0, 1)], axis=1
    )
    stride = min(4, devices)
    tokens = go_round(tokens, 1, stride)
    while stride < devices:
        steps = min(4, devices // stride)
        tokens = go_round(tokens, stride, steps)
        stride *= steps
    for offset in order[early:]:
        units = gather_units(scalars, kv, offset, parts_of(offset), head_count, True)
        arrived[offset] = [lax.ppermute(part, "wide", pairs_of(offset)) for part in units]
    arrived[0] = gather_units(scalars, kv, 0, [per_device], head_count, True)
    own_slots = lax.dynamic_slice_in_dim(decode_slot_pair, rank * per_device, per_device)
    rows = ((own_slots // per_device) ^ rank) * per_device + own_slots % per_device
    own_tokens = jnp.take(tokens, rows, axis=0)

    carry = None
    for offset in [0, *order]:
        done = 0
        for part in arrived[offset]:
            active = range(done, done + part.shape[0])
            done = active.stop
            last = offset == order[-1] and done == per_device
            carry = absorb(
                scalars,
                part,
                own_tokens,
                carry,
                offset,
                head_count,
                devices,
                dense[offset],
                last,
                active,
            )
    return tuple(carry)


def solution(mesh):
    in_specs = (
        P(None, "grp", None, "wide", None),
        P(("grp", "wide"), None),
        P(None, ("grp", "wide"), None),
        P("grp"),
        P("grp"),
    )
    out_specs = (P(None, ("grp", "wide"), None, None), P(("grp", "wide"), None))

    return jax.shard_map(local, mesh=mesh, in_specs=in_specs, out_specs=out_specs, check_vma=False)
```
